32 devices in a mesh: dp: 2 (over x), kvh: 4 (over z), seq: 4 (over y, core).
Axes of the slice: x: 2, y: 2, z: 4, core: 2. Of those that a mesh axis runs over, the one named last changes fastest.
Arguments:
- x_hidden: bfloat16 [64, 12288], P('dp'), parts along dimension 0
- seq_lens: int32 [64], P('dp'), parts along dimension 0
- k_cache: bfloat16 [64, 2048, 8, 128], P('dp', 'seq', 'kvh'), parts along dimension 0
- v_cache: bfloat16 [64, 2048, 8, 128], P('dp', 'seq', 'kvh'), parts along dimension 0
- w_q: bfloat16 [12288, 96, 128], P(None, ('kvh', 'seq'))
- w_o: bfloat16 [96, 128, 12288], P(('kvh', 'seq'))
Outputs:
- output: bfloat16 [64, 12288], P('dp'), parts along dimension 0
There are 2 independent parts. The reference program is written for one: setup_inputs(seed, part) draws one part's arguments, and reference() takes and returns one part's arrays. A program takes and returns all parts, laid end to end along the dimension named above; an argument that names none is the same for every part.
All inputs are finite; a program needn't handle non-finite values.
Results may differ from the reference program's by a relative error of at most 0.0034335.
Values are sent between devices in bfloat16 or wider.
A program may use at most 1 GiB of HBM per device.

```python
import jax
import jax.numpy as jnp
from jax import lax

BATCH_ROWS = 32
SEQ_LEN = 2048
MODEL_DIM = 12288
QUERY_HEADS = 96
KV_HEADS = 8
HEAD_DIM = 128
ROPE_THETA = 500000
TOKEN_SEGMENTS = 64


def rotate_query(q_raw, seq_lens):
    half_dim = HEAD_DIM // 2
    inv_freq = jnp.power(float(ROPE_THETA), -jnp.arange(half_dim, dtype=jnp.float32) * (2.0 / HEAD_DIM))
    angle = (seq_lens - 1).astype(jnp.float32)[:, None] * inv_freq[None, :]
    cosine = jnp.cos(angle)[:, None, :]
    sine = jnp.sin(angle)[:, None, :]
    first = q_raw[..., :half_dim]
    second = q_raw[..., half_dim:]
    return jnp.concatenate([first * cosine - second * sine, second * cosine + first * sine], axis=-1)


def setup_inputs(seed: int = 0, part: int = 0) -> dict:
    base_key = jax.random.key(seed)
    key_list = jax.random.split(base_key, 4)
    part_list = jax.random.split(jax.random.fold_in(key_list[0], part), 8)
    seg_len = SEQ_LEN // TOKEN_SEGMENTS
    low_len = SEQ_LEN // 4
    x_hidden = jax.random.normal(part_list[0], (BATCH_ROWS, MODEL_DIM), jnp.float32).astype(jnp.bfloat16)
    seq_lens = jax.random.randint(part_list[1], (BATCH_ROWS,), low_len, SEQ_LEN + 1)
    seq_lens = seq_lens.at[0].set(SEQ_LEN).at[1].set(low_len)
    seq_lens = jax.random.permutation(part_list[2], seq_lens)
    noise_shape = (BATCH_ROWS, TOKEN_SEGMENTS, seg_len, KV_HEADS, HEAD_DIM)
    mean_shape = (BATCH_ROWS, TOKEN_SEGMENTS, 1, KV_HEADS, HEAD_DIM)
    key_mean = 1.5 * jax.random.normal(part_list[3], mean_shape, jnp.float32)
    key_noise = jax.random.normal(part_list[4], noise_shape, jnp.float32)
    k_cache = (key_noise + key_mean).reshape(BATCH_ROWS, SEQ_LEN, KV_HEADS, HEAD_DIM).astype(jnp.bfloat16)
    value_mean = jax.random.normal(part_list[5], mean_shape, jnp.float32)
    value_noise = 0.7 * jax.random.normal(part_list[6], noise_shape, jnp.float32)
    v_cache = (value_noise + value_mean).reshape(BATCH_ROWS, SEQ_LEN, KV_HEADS, HEAD_DIM).astype(jnp.bfloat16)
    w_q = (jax.random.normal(key_list[1], (MODEL_DIM, QUERY_HEADS, HEAD_DIM), jnp.float32) * MODEL_DIM ** -0.5).astype(jnp.bfloat16)
    w_o = (jax.random.normal(key_list[2], (QUERY_HEADS, HEAD_DIM, MODEL_DIM), jnp.float32) * (QUERY_HEADS * HEAD_DIM) ** -0.5).astype(jnp.bfloat16)
    return dict(x_hidden=x_hidden, seq_lens=seq_lens, k_cache=k_cache, v_cache=v_cache, w_q=w_q, w_o=w_o)


def reference(x_hidden, seq_lens, k_cache, v_cache, w_q, w_o):
    group_size = QUERY_HEADS // KV_HEADS
    q_raw = jnp.einsum('bd,dhk->bhk', x_hidden.astype(jnp.float32), w_q.astype(jnp.float32))
    q_rot = rotate_query(q_raw, seq_lens).astype(jnp.bfloat16)
    q_flat = q_rot.reshape(BATCH_ROWS * KV_HEADS, group_size, HEAD_DIM)
    k_flat = k_cache.transpose(0, 2, 1, 3).reshape(BATCH_ROWS * KV_HEADS, SEQ_LEN, HEAD_DIM)
    v_flat = v_cache.transpose(0, 2, 1, 3).reshape(BATCH_ROWS * KV_HEADS, SEQ_LEN, HEAD_DIM)
    len_flat = jnp.repeat(seq_lens, KV_HEADS)
    positions = jnp.arange(SEQ_LEN)

    def one_head(operands):
        q_head, k_head, v_head, length = operands
        scores = jnp.dot(q_head, k_head.T, preferred_element_type=jnp.float32) * (HEAD_DIM ** -0.5)
        valid_mask = positions[None, :] < length
        scores = jnp.where(valid_mask, scores, -jnp.inf)
        weights = jnp.exp(scores - jnp.max(scores, axis=-1, keepdims=True))
        weight_sum = jnp.sum(weights, axis=-1, keepdims=True)
        attn = jnp.dot(weights.astype(jnp.bfloat16), v_head, preferred_element_type=jnp.float32) / weight_sum
        return attn.astype(jnp.bfloat16)

    attn = lax.map(one_head, (q_flat, k_flat, v_flat, len_flat)).reshape(BATCH_ROWS, QUERY_HEADS, HEAD_DIM)
    y_sum = jnp.einsum('bhk,hkd->bd', attn.astype(jnp.float32), w_o.astype(jnp.float32))
    return (x_hidden.astype(jnp.float32) + y_sum).astype(jnp.bfloat16)
```

```python
import functools

import jax
import jax.numpy as jnp
import numpy as np
from jax import lax
from jax.experimental import pallas as pl
from jax.experimental.pallas import tpu as pltpu
from jax.sharding import PartitionSpec as P

ROPE_THETA = 500000.0
MESH = pl.DeviceIdType.MESH
F32 = jnp.float32
BF16 = jnp.bfloat16

ROWS = 32
DIM = 12288
HEADS = 6
HD = 128
SEQ = 4
KVH = 4
T_DEV = 512
TN = 2 * T_DEV
KC = 4
KD = DIM // KC
AHEAD = 7
VMEM_LIMIT = 60 * 2 ** 20
SLOTS = 8
BC = 8
NB = ROWS // BC
HALF = ROWS // 2
PITCH = 40
GROUP = 2
BLK = DIM // 8


def kernel(x_h, len_h, freq_h, k_h, v_h, wq_h, wo_h, out_ref,
           x_s, len_s, freq_s, wq_s, k_s, v_s, wo_s,
           posq, qg, q_t, ob, mlb, rb, attn_s, ypart, yrecv, yrecv2, zrecv,
           in_sem, wq_sem, k_sem, v_sem, wo_sem,
           qs_sem, qr_sem, cs_sem, cr_sem,
           ds_sem, dr_sem, ys_sem, yr_sem, zs_sem, zr_sem,
           azs_sem, azr_sem, ays_sem, ayr_sem, ads_sem, adr_sem, turn_sem):
    d = lax.axis_index('dp')
    z = lax.axis_index('kvh')
    me = lax.axis_index('seq')
    core = lax.rem(me, 2)
    y = lax.div(me, 2)

    def seq_peer(i):
        c = 1 - core if i & 1 else core
        yy = 1 - y if i & 2 else y
        return yy * 2 + c

    zs = [lax.rem(z + i, KVH) for i in (2, 1, 3, 0)]
    blocks = [zz * 2 + (1 - y) for zz in zs] + [zz * 2 + y for zz in zs]

    x_cp = pltpu.make_async_copy(x_h, x_s, in_sem.at[0])
    len_cp = pltpu.make_async_copy(len_h, len_s, in_sem.at[1])
    freq_cp = pltpu.make_async_copy(freq_h, freq_s, in_sem.at[2])
    len_cp.start()
    freq_cp.start()
    x_cp.start()

    def wq_cp(p, c):
        n = p * KC + c
        src = wq_h.at[pl.ds(2 * p, 2), pl.ds(c * KD, KD)]
        return pltpu.make_async_copy(src, wq_s.at[n % SLOTS], wq_sem.at[n])

    def k_cp(j):
        at = pl.ds(j * BC, BC)
        return pltpu.make_async_copy(k_h.at[at], k_s.at[at], k_sem.at[j])

    def v_cp(j):
        at = pl.ds(j * BC, BC)
        return pltpu.make_async_copy(v_h.at[at], v_s.at[at], v_sem.at[j])

    def wo_cp(i):
        src = wo_h.at[:, pl.ds(pl.multiple_of(blocks[i] * BLK, BLK), BLK)]
        return pltpu.make_async_copy(src, wo_s.at[i], wo_sem.at[i])

    fetches = [wq_cp(p, c) for p in range(3) for c in range(KC)]
    for j in range(NB):
        fetches += [k_cp(j), v_cp(j)]
    for cp in fetches[:AHEAD]:
        cp.start(priority=1)

    barrier = pltpu.get_barrier_semaphore()
    for i in range(1, SEQ):
        pl.semaphore_signal(barrier, inc=1, device_id=(d, z, seq_peer(i)), device_id_type=MESH)
    for i in range(1, KVH):
        pl.semaphore_signal(barrier, inc=1, device_id=(d, lax.rem(z + i, KVH), me), device_id_type=MESH)

    q_t[...] = jnp.zeros_like(q_t)
    lane = lax.broadcasted_iota(jnp.int32, (ROWS, TN), 1)
    row = lax.broadcasted_iota(jnp.int32, (ROWS, TN), 0)
    mine = (lane & 1) == (row >> 4)
    posq[...] = jnp.where(mine, me * T_DEV + (lane >> 1), 1 << 30)
    len_cp.wait()
    freq_cp.wait()
    rows128 = lax.broadcasted_iota(jnp.int32, (ROWS, HD), 0)
    lane128 = lax.broadcasted_iota(jnp.int32, (ROWS, HD), 1)
    pos = jnp.zeros((ROWS, HD), jnp.int32)
    for b in range(ROWS):
        pos = jnp.where(rows128 == b, len_s[b] - 1, pos)
    angle = pos.astype(F32) * freq_s[0:1, :]
    cosine = jnp.cos(angle)
    sine = jnp.sin(angle)
    sine = jnp.where(lane128 < HD // 2, -sine, sine)

    def q_copy(p, i, slot):
        at = (slot, pl.ds(2 * p, 2))
        return pltpu.make_async_remote_copy(
            src_ref=qg.at[at], dst_ref=qg.at[at],
            send_sem=qs_sem.at[p, i - 1], recv_sem=qr_sem.at[p, i - 1],
            device_id=(d, z, seq_peer(i)), device_id_type=MESH)

    x_cp.wait()
    for p in range(3):
        acc = [jnp.zeros((ROWS, HD), F32)] * 2
        for c in range(KC):
            n = p * KC + c
            wq_cp(p, c).wait()
            fetches[n + AHEAD].start(priority=1)
            at = slice(c * KD, (c + 1) * KD)
            for u in range(2):
                acc[u] = acc[u] + jnp.dot(x_s[:, at], wq_s[n % SLOTS, u], preferred_element_type=F32)
        for u in range(2):
            q = acc[u]
            q = q * cosine + pltpu.roll(q, HD // 2, axis=1) * sine
            qg[me, 2 * p + u] = q.astype(BF16)
        if p == 0:
            pl.semaphore_wait(barrier, SEQ - 1 + KVH - 1)
        for i in range(1, SEQ):
            q_copy(p, i, me).start()
    for cp in fetches[3 * KC + AHEAD:] + [wo_cp(0)]:
        cp.start(priority=1)
    for p in range(3):
        for i in range(1, SEQ):
            q_copy(p, i, seq_peer(i)).wait_recv()
    for i in range(1, 8):
        wo_cp(i).start(priority=1)
    q_rows = q_t.reshape(ROWS * PITCH, HD)
    for s in range(SEQ):
        for h in range(HEADS):
            q_rows[pl.ds(s * 8 + h, ROWS, stride=PITCH), :] = qg[s, h].astype(F32)

    ob_rows = ob.reshape(32 * ROWS, HD)
    ml_rows = mlb.reshape(ROWS * PITCH, HD)
    scale = HD ** -0.5

    def c_copy(j, i, dst, slot):
        at = pl.ds(j * BC, BC)
        return pltpu.make_async_remote_copy(
            src_ref=ob.at[at, dst], dst_ref=rb.at[slot, at],
            send_sem=cs_sem.at[j, i - 1], recv_sem=cr_sem.at[j, i - 1],
            device_id=(d, z, seq_peer(i)), device_id_type=MESH)

    lane8 = lax.broadcasted_iota(jnp.int32, (BC, HD), 1)
    lane32 = lax.broadcasted_iota(jnp.int32, (32, HD), 1)

    def piece(j, carry):
        k_cp(j).wait()
        v_cp(j).wait()
        for g in range(BC // 4):
            ws = []
            for h in range(2):
                b = j * BC + g * 4 + 2 * h
                qa, qb = q_t[b, :32].astype(BF16), q_t[b + 1, :32].astype(BF16)
                zero = jnp.zeros_like(qa)
                lhs = jnp.concatenate([jnp.concatenate([qa, zero], axis=1), jnp.concatenate([zero, qb], axis=1)], axis=0)
                rhs = jnp.concatenate([k_s[b], k_s[b + 1]], axis=1)
                both = lax.dot_general(lhs, rhs, (((1,), (1,)), ((), ())), preferred_element_type=F32)
                for u in range(2):
                    s = both[u * 32:(u + 1) * 32]
                    s = jnp.where(posq[...] < len_s[b + u], s * scale, -jnp.inf)
                    m = jnp.max(s, axis=1, keepdims=True)
                    w = jnp.exp(s - jnp.where(m == -jnp.inf, 0.0, m))
                    l = jnp.sum(w, axis=1, keepdims=True)
                    mlb[b + u, :32] = jnp.where(lane32 < 64, m, l)
                    ws.append(w.astype(BF16))
            b = j * BC + g * 4
            rhs = jnp.concatenate([v_s[b + u] for u in range(4)], axis=1)
            out = jnp.dot(jnp.concatenate(ws, axis=0), rhs, preferred_element_type=F32)
            for u in range(4):
                for v in range(SEQ):
                    ob[b + u, v] = out[u * 32 + v * 8:u * 32 + (v + 1) * 8, u * HD:(u + 1) * HD]
        for v in range(SEQ):
            stat = jnp.zeros((BC, HD), F32)
            for h in range(HEADS):
                of_head = ml_rows[pl.ds(j * BC * PITCH + v * 8 + h, BC, stride=PITCH), :]
                stat = jnp.where((lane8 & 63) == h, of_head, stat)
            ob_rows[pl.ds(j * BC * 32 + v * 8 + HEADS, BC, stride=32), :] = stat
        for i in range(1, SEQ):
            c_copy(j, i, seq_peer(i), me).start()
        return carry

    lax.fori_loop(0, NB, piece, 0)
    for p in range(3):
        for i in range(1, SEQ):
            q_copy(p, i, me).wait_send()
    def combine(half):
        for j in range(half * NB // 2, (half + 1) * NB // 2):
            for i in range(1, SEQ):
                c_copy(j, i, seq_peer(i), seq_peer(i)).wait_recv()
        at = pl.ds(half * HALF, HALF)
        rb_rows = rb.reshape(SEQ * ROWS * 8, HD)

        def part(i, h):
            if i == 0:
                return ob_rows[pl.ds(half * HALF * 32 + me * 8 + h, HALF, stride=32), :]
            return rb_rows[pl.ds((seq_peer(i) * ROWS + half * HALF) * 8 + h, HALF, stride=8), :]

        stats = [part(i, HEADS) for i in range(SEQ)]
        top = functools.reduce(jnp.maximum, stats)
        fac = [jnp.exp(st - top) for st in stats]
        total = functools.reduce(jnp.add, [f * pltpu.roll(st, 64, axis=1) for f, st in zip(fac, stats)])
        for h in range(HEADS):
            o = functools.reduce(jnp.add, [part(i, h) * f[:, h:h + 1] for i, f in enumerate(fac)])
            attn_s[at, h * HD:(h + 1) * HD] = (o / total[:, h:h + 1]).astype(BF16)

    def d_copy(half, n):
        return pltpu.make_async_remote_copy(
            src_ref=ypart.at[half, n], dst_ref=yrecv.at[n], send_sem=ds_sem.at[n], recv_sem=dr_sem.at[n],
            device_id=(d, z, seq_peer(1)), device_id_type=MESH)

    def y_copy(n):
        return pltpu.make_async_remote_copy(
            src_ref=ypart.at[core, n], dst_ref=yrecv2.at[n], send_sem=ys_sem.at[n], recv_sem=yr_sem.at[n],
            device_id=(d, z, seq_peer(2)), device_id_type=MESH)

    def z_copy(n, to, slot):
        return pltpu.make_async_remote_copy(
            src_ref=ypart.at[core, 4 + n], dst_ref=zrecv.at[slot], send_sem=zs_sem.at[n], recv_sem=zr_sem.at[slot],
            device_id=(d, to, me), device_id_type=MESH)

    def y_step(n):
        y_copy(n).wait_recv()
        ypart[core, 4 + n] = ypart[core, 4 + n] + yrecv2[n]
        if n < 3:
            z_copy(n, zs[n], z).start()

    def d_step(half, n):
        for u in range(n, n + GROUP):
            d_copy(half, u).wait_recv()
            ypart[half, u] = ypart[half, u] + yrecv[u]
            if u < 4:
                y_copy(u).start()

    for half in range(2):
        combine(half)
        for n in range(0, 8 + GROUP, GROUP):
            if n < 8:
                if half == 0:
                    for u in range(n, n + GROUP):
                        wo_cp(u).wait()
                for u in range(n, n + GROUP):
                    ypart[half, u] = jnp.dot(attn_s[half * HALF:(half + 1) * HALF, :], wo_s[u],
                                             preferred_element_type=F32)

                @pl.when(core != half)
                def _():
                    for u in range(n, n + GROUP):
                        d_copy(half, u).start()
            if 0 < n <= 4 or (n > 4 and half == 1):
                @pl.when(core == half)
                def _():
                    d_step(half, n - GROUP)
            if half == 1 and n in (2, 4):
                @pl.when(core == 0)
                def _():
                    d_step(0, n + 2)
            if half == 1 and n >= 4:
                @pl.when(core == 0)
                def _():
                    y_step((n - 4) // 2)

    @pl.when(core == 0)
    def _():
        y_step(3)

    @pl.when(core == 1)
    def _():
        for n in range(4):
            y_step(n)
        for n in range(3):
            z_copy(n, zs[n], z).wait_send()
        pl.semaphore_signal(turn_sem, inc=1, device_id=(d, z, seq_peer(1)), device_id_type=MESH)

    def block_at(half, block):
        return (pl.ds(pl.multiple_of(half * HALF, HALF), HALF), pl.ds(pl.multiple_of(block * BLK, BLK), BLK))

    def ag_z(i, block, to, frm):
        at = block_at(core, block)
        return pltpu.make_async_remote_copy(
            src_ref=out_ref.at[at], dst_ref=out_ref.at[at], send_sem=azs_sem.at[i], recv_sem=azr_sem.at[frm],
            device_id=(d, to, me), device_id_type=MESH)

    def ag_y(block, zz):
        at = block_at(core, block)
        return pltpu.make_async_remote_copy(
            src_ref=out_ref.at[at], dst_ref=out_ref.at[at], send_sem=ays_sem.at[zz], recv_sem=ayr_sem.at[zz],
            device_id=(d, z, seq_peer(2)), device_id_type=MESH)

    def ag_d(half, block):
        at = block_at(half, block)
        return pltpu.make_async_remote_copy(
            src_ref=out_ref.at[at], dst_ref=out_ref.at[at], send_sem=ads_sem.at[block], recv_sem=adr_sem.at[block],
            device_id=(d, z, seq_peer(1)), device_id_type=MESH)

    for n in range(3):
        z_copy(n, zs[n], zs[n]).wait_recv()
    own = z * 2 + y
    at = block_at(core, own)
    f = ypart[core, 7] + zrecv[zs[0]] + zrecv[zs[1]] + zrecv[zs[2]]
    out_ref[at] = (x_s[at].astype(F32) + f).astype(BF16)
    ag_d(core, own).start()

    @pl.when(core == 0)
    def _():
        pl.semaphore_wait(turn_sem, 1)

    for n in range(3):
        ag_z(n, own, zs[n], z).start()
    ag_y(own, z).start()
    for n in (1, 2, 0):
        b = zs[n] * 2 + y
        ag_z(n, b, zs[n], zs[n]).wait_recv()
        ag_y(b, zs[n]).start()
        ag_d(core, b).start()
    for zz in (z, zs[1], zs[2], zs[0]):
        b = zz * 2 + (1 - y)
        ag_y(b, zz).wait_recv()
        ag_d(core, b).start()
    for n in range(8):
        ag_d(1 - core, n).wait_recv()

    for j in range(NB):
        for i in range(1, SEQ):
            c_copy(j, i, seq_peer(i), me).wait_send()
    for n in range(8):
        d_copy(0, n).wait_send()
        ag_d(core, n).wait_send()
    for n in range(4):
        y_copy(n).wait_send()
        ag_y(n * 2 + y, n).wait_send()
    @pl.when(core == 0)
    def _():
        for n in range(3):
            z_copy(n, zs[n], z).wait_send()

    for n in range(3):
        ag_z(n, own, zs[n], z).wait_send()


def solution(mesh):
    half = HD // 2
    freq = ROPE_THETA ** (-np.arange(half, dtype=np.float64) * (2.0 / HD))
    freq = np.tile(np.concatenate([freq, freq]).astype(np.float32), (8, 1))
    dma = pltpu.SemaphoreType.DMA

    def local_step(x_hidden, seq_lens, k_loc, v_loc, wq_loc, wo_loc):
        any_spec = pl.BlockSpec(memory_space=pl.ANY)
        return pl.pallas_call(
            kernel,
            out_shape=pltpu.VMEM((ROWS, DIM), BF16),
            in_specs=[any_spec] * 7,
            out_specs=pl.BlockSpec(memory_space=pltpu.VMEM),
            scratch_shapes=[
                pltpu.VMEM((ROWS, DIM), BF16),
                pltpu.SMEM((ROWS,), jnp.int32),
                pltpu.VMEM((8, HD), F32),
                pltpu.VMEM((SLOTS, 2, KD, HD), BF16),
                pltpu.VMEM((ROWS, TN, HD), BF16),
                pltpu.VMEM((ROWS, TN, HD), BF16),
                pltpu.VMEM((8, HEADS * HD, BLK), BF16),
                pltpu.VMEM((ROWS, TN), jnp.int32),
                pltpu.VMEM((SEQ, HEADS, ROWS, HD), BF16),
                pltpu.VMEM((ROWS, PITCH, HD), F32),
                pltpu.VMEM((ROWS, SEQ, 8, HD), F32),
                pltpu.VMEM((ROWS, PITCH, HD), F32),
                pltpu.VMEM((SEQ, ROWS, 8, HD), F32),
                pltpu.VMEM((ROWS, HEADS * HD), BF16),
                pltpu.VMEM((2, 8, HALF, BLK), F32),
                pltpu.VMEM((8, HALF, BLK), F32),
                pltpu.VMEM((4, HALF, BLK), F32),
                pltpu.VMEM((4, HALF, BLK), F32),
                dma((3,)), dma((3 * KC,)), dma((NB,)), dma((NB,)), dma((8,)),
                dma((3, 3)), dma((3, 3)), dma((NB, 3)), dma((NB, 3)),
                dma((8,)), dma((8,)), dma((4,)), dma((4,)), dma((3,)), dma((4,)),
                dma((3,)), dma((4,)), dma((4,)), dma((4,)), dma((8,)), dma((8,)),
                pltpu.SemaphoreType.REGULAR,
            ],
            compiler_params=pltpu.CompilerParams(
                collective_id=0, has_side_effects=True, vmem_limit_bytes=VMEM_LIMIT),
            name='decode_step',
        )(x_hidden, seq_lens, jnp.asarray(freq),
          k_loc.reshape(ROWS, TN, HD), v_loc.reshape(ROWS, TN, HD),
          wq_loc.transpose(1, 0, 2), wo_loc.reshape(HEADS * HD, DIM))

    return jax.shard_map(
        local_step,
        mesh=mesh,
        in_specs=(P('dp', None), P('dp'), P('dp', 'seq', 'kvh', None), P('dp', 'seq', 'kvh', None),
                  P(None, ('kvh', 'seq'), None), P(('kvh', 'seq'), None, None)),
        out_specs=P('dp', None),
        check_vma=False)
```

```python
import functools

import jax
import jax.numpy as jnp
import numpy as np
from jax import lax
from jax.experimental import pallas as pl
from jax.experimental.pallas import tpu as pltpu
from jax.sharding import PartitionSpec as P

ROPE_THETA = 500000.0
MESH = pl.DeviceIdType.MESH
F32 = jnp.float32
BF16 = jnp.bfloat16

ROWS = 32
DIM = 12288
HEADS = 6
HD = 128
SEQ = 4
KVH = 4
T_DEV = 512
TN = 2 * T_DEV
KC = 4
KD = DIM // KC
AHEAD = 7
VMEM_LIMIT = 60 * 2 ** 20
SLOTS = 8
BC = 8
NB = ROWS // BC
HALF = ROWS // 2
PITCH = 40
GROUP = 2
BLK = DIM // 8


def kernel(x_h, len_h, freq_h, k_h, v_h, wq_h, wo_h, out_ref,
           x_s, len_s, freq_s, wq_s, k_s, v_s, wo_s,
           posq, qg, q_t, ob, mlb, rb, attn_s, ypart, yrecv, yrecv2, zrecv,
           in_sem, wq_sem, k_sem, v_sem, wo_sem,
           qs_sem, qr_sem, cs_sem, cr_sem,
           ds_sem, dr_sem, ys_sem, yr_sem, zs_sem, zr_sem,
           azs_sem, azr_sem, ays_sem, ayr_sem, ads_sem, adr_sem, turn_sem):
    d = lax.axis_index('dp')
    z = lax.axis_index('kvh')
    me = lax.axis_index('seq')
    core = lax.rem(me, 2)
    y = lax.div(me, 2)

    def seq_peer(i):
        c = 1 - core if i & 1 else core
        yy = 1 - y if i & 2 else y
        return yy * 2 + c

    far = 1 - lax.div(z, 2)
    zs = [3 * far, 1 + far, z + 1 - 2 * lax.rem(z, 2), z]
    blocks = [zz * 2 + (1 - y) for zz in zs] + [zz * 2 + y for zz in zs]

    x_cp = pltpu.make_async_copy(x_h, x_s, in_sem.at[0])
    len_cp = pltpu.make_async_copy(len_h, len_s, in_sem.at[1])
    freq_cp = pltpu.make_async_copy(freq_h, freq_s, in_sem.at[2])
    len_cp.start()
    freq_cp.start()
    x_cp.start()

    def wq_cp(p, c):
        n = p * KC + c
        src = wq_h.at[pl.ds(2 * p, 2), pl.ds(c * KD, KD)]
        return pltpu.make_async_copy(src, wq_s.at[n % SLOTS], wq_sem.at[n])

    def k_cp(j):
        at = pl.ds(j * BC, BC)
        return pltpu.make_async_copy(k_h.at[at], k_s.at[at], k_sem.at[j])

    def v_cp(j):
        at = pl.ds(j * BC, BC)
        return pltpu.make_async_copy(v_h.at[at], v_s.at[at], v_sem.at[j])

    def wo_cp(i):
        src = wo_h.at[:, pl.ds(pl.multiple_of(blocks[i] * BLK, BLK), BLK)]
        return pltpu.make_async_copy(src, wo_s.at[i], wo_sem.at[i])

    fetches = [wq_cp(p, c) for p in range(3) for c in range(KC)]
    for j in range(NB):
        fetches += [k_cp(j), v_cp(j)]
    for cp in fetches[:AHEAD]:
        cp.start(priority=1)

    barrier = pltpu.get_barrier_semaphore()
    for i in range(1, SEQ):
        pl.semaphore_signal(barrier, inc=1, device_id=(d, z, seq_peer(i)), device_id_type=MESH)
    for i in range(1, KVH):
        pl.semaphore_signal(barrier, inc=1, device_id=(d, lax.rem(z + i, KVH), me), device_id_type=MESH)

    q_t[...] = jnp.zeros_like(q_t)
    lane = lax.broadcasted_iota(jnp.int32, (ROWS, TN), 1)
    row = lax.broadcasted_iota(jnp.int32, (ROWS, TN), 0)
    mine = (lane & 1) == (row >> 4)
    posq[...] = jnp.where(mine, me * T_DEV + (lane >> 1), 1 << 30)
    len_cp.wait()
    freq_cp.wait()
    rows128 = lax.broadcasted_iota(jnp.int32, (ROWS, HD), 0)
    lane128 = lax.broadcasted_iota(jnp.int32, (ROWS, HD), 1)
    pos = jnp.zeros((ROWS, HD), jnp.int32)
    for b in range(ROWS):
        pos = jnp.where(rows128 == b, len_s[b] - 1, pos)
    angle = pos.astype(F32) * freq_s[0:1, :]
    cosine = jnp.cos(angle)
    sine = jnp.sin(angle)
    sine = jnp.where(lane128 < HD // 2, -sine, sine)

    def q_copy(p, i, slot):
        at = (slot, pl.ds(2 * p, 2))
        return pltpu.make_async_remote_copy(
            src_ref=qg.at[at], dst_ref=qg.at[at],
            send_sem=qs_sem.at[p, i - 1], recv_sem=qr_sem.at[p, i - 1],
            device_id=(d, z, seq_peer(i)), device_id_type=MESH)

    x_cp.wait()
    for p in range(3):
        acc = [jnp.zeros((ROWS, HD), F32)] * 2
        for c in range(KC):
            n = p * KC + c
            wq_cp(p, c).wait()
            fetches[n + AHEAD].start(priority=1)
            at = slice(c * KD, (c + 1) * KD)
            for u in range(2):
                acc[u] = acc[u] + jnp.dot(x_s[:, at], wq_s[n % SLOTS, u], preferred_element_type=F32)
        for u in range(2):
            q = acc[u]
            q = q * cosine + pltpu.roll(q, HD // 2, axis=1) * sine
            qg[me, 2 * p + u] = q.astype(BF16)
        if p == 0:
            pl.semaphore_wait(barrier, SEQ - 1 + KVH - 1)
        for i in range(1, SEQ):
            q_copy(p, i, me).start()
    for cp in fetches[3 * KC + AHEAD:] + [wo_cp(0)]:
        cp.start(priority=1)
    for p in range(3):
        for i in range(1, SEQ):
            q_copy(p, i, seq_peer(i)).wait_recv()
    for i in range(1, 8):
        wo_cp(i).start(priority=1)
    q_rows = q_t.reshape(ROWS * PITCH, HD)
    for s in range(SEQ):
        for h in range(HEADS):
            q_rows[pl.ds(s * 8 + h, ROWS, stride=PITCH), :] = qg[s, h].astype(F32)

    ob_rows = ob.reshape(32 * ROWS, HD)
    ml_rows = mlb.reshape(ROWS * PITCH, HD)
    scale = HD ** -0.5

    def c_copy(j, i, dst, slot):
        at = pl.ds(j * BC, BC)
        return pltpu.make_async_remote_copy(
            src_ref=ob.at[at, dst], dst_ref=rb.at[slot, at],
            send_sem=cs_sem.at[j, i - 1], recv_sem=cr_sem.at[j, i - 1],
            device_id=(d, z, seq_peer(i)), device_id_type=MESH)

    lane8 = lax.broadcasted_iota(jnp.int32, (BC, HD), 1)
    lane32 = lax.broadcasted_iota(jnp.int32, (32, HD), 1)

    def piece(j, carry):
        k_cp(j).wait()
        v_cp(j).wait()
        for g in range(BC // 4):
            ws = []
            for h in range(2):
                b = j * BC + g * 4 + 2 * h
                qa, qb = q_t[b, :32].astype(BF16), q_t[b + 1, :32].astype(BF16)
                zero = jnp.zeros_like(qa)
                lhs = jnp.concatenate([jnp.concatenate([qa, zero], axis=1), jnp.concatenate([zero, qb], axis=1)], axis=0)
                rhs = jnp.concatenate([k_s[b], k_s[b + 1]], axis=1)
                both = lax.dot_general(lhs, rhs, (((1,), (1,)), ((), ())), preferred_element_type=F32)
                for u in range(2):
                    s = both[u * 32:(u + 1) * 32]
                    s = jnp.where(posq[...] < len_s[b + u], s * scale, -jnp.inf)
                    m = jnp.max(s, axis=1, keepdims=True)
                    w = jnp.exp(s - jnp.where(m == -jnp.inf, 0.0, m))
                    l = jnp.sum(w, axis=1, keepdims=True)
                    mlb[b + u, :32] = jnp.where(lane32 < 64, m, l)
                    ws.append(w.astype(BF16))
            for u in range(4):
                b = j * BC + g * 4 + u
                out = jnp.dot(ws[u], v_s[b], preferred_element_type=F32)
                for v in range(SEQ):
                    ob[b, v] = out[v * 8:(v + 1) * 8]
        for v in range(SEQ):
            stat = jnp.zeros((BC, HD), F32)
            for h in range(HEADS):
                of_head = ml_rows[pl.ds(j * BC * PITCH + v * 8 + h, BC, stride=PITCH), :]
                stat = jnp.where((lane8 & 63) == h, of_head, stat)
            ob_rows[pl.ds(j * BC * 32 + v * 8 + HEADS, BC, stride=32), :] = stat
        for i in range(1, SEQ):
            c_copy(j, i, seq_peer(i), me).start()
        return carry

    lax.fori_loop(0, NB, piece, 0)
    for p in range(3):
        for i in range(1, SEQ):
            q_copy(p, i, me).wait_send()
    def combine(half):
        for j in range(half * NB // 2, (half + 1) * NB // 2):
            for i in range(1, SEQ):
                c_copy(j, i, seq_peer(i), seq_peer(i)).wait_recv()
        at = pl.ds(half * HALF, HALF)
        rb_rows = rb.reshape(SEQ * ROWS * 8, HD)

        def part(i, h):
            if i == 0:
                return ob_rows[pl.ds(half * HALF * 32 + me * 8 + h, HALF, stride=32), :]
            return rb_rows[pl.ds((seq_peer(i) * ROWS + half * HALF) * 8 + h, HALF, stride=8), :]

        stats = [part(i, HEADS) for i in range(SEQ)]
        top = functools.reduce(jnp.maximum, stats)
        fac = [jnp.exp(st - top) for st in stats]
        total = functools.reduce(jnp.add, [f * pltpu.roll(st, 64, axis=1) for f, st in zip(fac, stats)])
        for h in range(HEADS):
            o = functools.reduce(jnp.add, [part(i, h) * f[:, h:h + 1] for i, f in enumerate(fac)])
            attn_s[at, h * HD:(h + 1) * HD] = (o / total[:, h:h + 1]).astype(BF16)

    def d_copy(half, n):
        return pltpu.make_async_remote_copy(
            src_ref=ypart.at[half, n], dst_ref=yrecv.at[n], send_sem=ds_sem.at[n], recv_sem=dr_sem.at[n],
            device_id=(d, z, seq_peer(1)), device_id_type=MESH)

    def y_copy(n):
        return pltpu.make_async_remote_copy(
            src_ref=ypart.at[core, n], dst_ref=yrecv2.at[n], send_sem=ys_sem.at[n], recv_sem=yr_sem.at[n],
            device_id=(d, z, seq_peer(2)), device_id_type=MESH)

    def z_copy(n, to, slot):
        return pltpu.make_async_remote_copy(
            src_ref=ypart.at[core, 4 + n], dst_ref=zrecv.at[slot], send_sem=zs_sem.at[n], recv_sem=zr_sem.at[slot],
            device_id=(d, to, me), device_id_type=MESH)

    def y_step(n):
        y_copy(n).wait_recv()
        ypart[core, 4 + n] = ypart[core, 4 + n] + yrecv2[n]
        if n < 3:
            z_copy(n, zs[n], z).start()

    def d_step(half, n):
        for u in range(n, n + GROUP):
            d_copy(half, u).wait_recv()
            ypart[half, u] = ypart[half, u] + yrecv[u]
            if u < 4:
                y_copy(u).start()

    for half in range(2):
        combine(half)
        for n in range(0, 8 + GROUP, GROUP):
            if n < 8:
                if half == 0:
                    for u in range(n, n + GROUP):
                        wo_cp(u).wait()
                for u in range(n, n + GROUP):
                    ypart[half, u] = jnp.dot(attn_s[half * HALF:(half + 1) * HALF, :], wo_s[u],
                                             preferred_element_type=F32)

                @pl.when(core != half)
                def _():
                    for u in range(n, n + GROUP):
                        d_copy(half, u).start()
            if 0 < n <= 4 or (n > 4 and half == 1):
                @pl.when(core == half)
                def _():
                    d_step(half, n - GROUP)
            if half == 1 and n in (2, 4):
                @pl.when(core == 0)
                def _():
                    d_step(0, n + 2)
            if half == 1 and n >= 4:
                @pl.when(core == 0)
                def _():
                    y_step((n - 4) // 2)

    @pl.when(core == 0)
    def _():
        y_step(3)

    @pl.when(core == 1)
    def _():
        for n in range(4):
            y_step(n)
        for n in range(3):
            z_copy(n, zs[n], z).wait_send()
        pl.semaphore_signal(turn_sem, inc=1, device_id=(d, z, seq_peer(1)), device_id_type=MESH)

    def block_at(half, block):
        return (pl.ds(pl.multiple_of(half * HALF, HALF), HALF), pl.ds(pl.multiple_of(block * BLK, BLK), BLK))

    def ag_z(i, block, to, frm):
        at = block_at(core, block)
        return pltpu.make_async_remote_copy(
            src_ref=out_ref.at[at], dst_ref=out_ref.at[at], send_sem=azs_sem.at[i], recv_sem=azr_sem.at[frm],
            device_id=(d, to, me), device_id_type=MESH)

    def ag_y(block, zz):
        at = block_at(core, block)
        return pltpu.make_async_remote_copy(
            src_ref=out_ref.at[at], dst_ref=out_ref.at[at], send_sem=ays_sem.at[zz], recv_sem=ayr_sem.at[zz],
            device_id=(d, z, seq_peer(2)), device_id_type=MESH)

    def ag_d(half, block):
        at = block_at(half, block)
        return pltpu.make_async_remote_copy(
            src_ref=out_ref.at[at], dst_ref=out_ref.at[at], send_sem=ads_sem.at[block], recv_sem=adr_sem.at[block],
            device_id=(d, z, seq_peer(1)), device_id_type=MESH)

    for n in range(3):
        z_copy(n, zs[n], zs[n]).wait_recv()
    own = z * 2 + y
    at = block_at(core, own)
    f = ypart[core, 7] + zrecv[zs[0]] + zrecv[zs[1]] + zrecv[zs[2]]
    out_ref[at] = (x_s[at].astype(F32) + f).astype(BF16)
    ag_d(core, own).start()

    @pl.when(core == 0)
    def _():
        pl.semaphore_wait(turn_sem, 1)

    az = [lax.rem(z + i, KVH) for i in (1, 3, 2)]
    for n in range(3):
        ag_z(n, own, az[n], z).start()
    ag_y(own, z).start()
    for n in (0, 1, 2):
        b = az[n] * 2 + y
        ag_z(n, b, az[n], az[n]).wait_recv()
        ag_y(b, az[n]).start()
        ag_d(core, b).start()
    for zz in (z, az[0], az[1], az[2]):
        b = zz * 2 + (1 - y)
        ag_y(b, zz).wait_recv()
        ag_d(core, b).start()
    for n in range(8):
        ag_d(1 - core, n).wait_recv()

    for j in range(NB):
        for i in range(1, SEQ):
            c_copy(j, i, seq_peer(i), me).wait_send()
    for n in range(8):
        d_copy(0, n).wait_send()
        ag_d(core, n).wait_send()
    for n in range(4):
        y_copy(n).wait_send()
        ag_y(n * 2 + y, n).wait_send()
    @pl.when(core == 0)
    def _():
        for n in range(3):
            z_copy(n, zs[n], z).wait_send()

    for n in range(3):
        ag_z(n, own, az[n], z).wait_send()


def solution(mesh):
    half = HD // 2
    freq = ROPE_THETA ** (-np.arange(half, dtype=np.float64) * (2.0 / HD))
    freq = np.tile(np.concatenate([freq, freq]).astype(np.float32), (8, 1))
    dma = pltpu.SemaphoreType.DMA

    def local_step(x_hidden, seq_lens, k_loc, v_loc, wq_loc, wo_loc):
        any_spec = pl.BlockSpec(memory_space=pl.ANY)
        return pl.pallas_call(
            kernel,
            out_shape=pltpu.VMEM((ROWS, DIM), BF16),
            in_specs=[any_spec] * 7,
            out_specs=pl.BlockSpec(memory_space=pltpu.VMEM),
            scratch_shapes=[
                pltpu.VMEM((ROWS, DIM), BF16),
                pltpu.SMEM((ROWS,), jnp.int32),
                pltpu.VMEM((8, HD), F32),
                pltpu.VMEM((SLOTS, 2, KD, HD), BF16),
                pltpu.VMEM((ROWS, TN, HD), BF16),
                pltpu.VMEM((ROWS, TN, HD), BF16),
                pltpu.VMEM((8, HEADS * HD, BLK), BF16),
                pltpu.VMEM((ROWS, TN), jnp.int32),
                pltpu.VMEM((SEQ, HEADS, ROWS, HD), BF16),
                pltpu.VMEM((ROWS, PITCH, HD), F32),
                pltpu.VMEM((ROWS, SEQ, 8, HD), F32),
                pltpu.VMEM((ROWS, PITCH, HD), F32),
                pltpu.VMEM((SEQ, ROWS, 8, HD), F32),
                pltpu.VMEM((ROWS, HEADS * HD), BF16),
                pltpu.VMEM((2, 8, HALF, BLK), F32),
                pltpu.VMEM((8, HALF, BLK), F32),
                pltpu.VMEM((4, HALF, BLK), F32),
                pltpu.VMEM((4, HALF, BLK), F32),
                dma((3,)), dma((3 * KC,)), dma((NB,)), dma((NB,)), dma((8,)),
                dma((3, 3)), dma((3, 3)), dma((NB, 3)), dma((NB, 3)),
                dma((8,)), dma((8,)), dma((4,)), dma((4,)), dma((3,)), dma((4,)),
                dma((3,)), dma((4,)), dma((4,)), dma((4,)), dma((8,)), dma((8,)),
                pltpu.SemaphoreType.REGULAR,
            ],
            compiler_params=pltpu.CompilerParams(
                collective_id=0, has_side_effects=True, vmem_limit_bytes=VMEM_LIMIT),
            name='decode_step',
        )(x_hidden, seq_lens, jnp.asarray(freq),
          k_loc.reshape(ROWS, TN, HD), v_loc.reshape(ROWS, TN, HD),
          wq_loc.transpose(1, 0, 2), wo_loc.reshape(HEADS * HD, DIM))

    return jax.shard_map(
        local_step,
        mesh=mesh,
        in_specs=(P('dp', None), P('dp'), P('dp', 'seq', 'kvh', None), P('dp', 'seq', 'kvh', None),
                  P(None, ('kvh', 'seq'), None), P(('kvh', 'seq'), None, None)),
        out_specs=P('dp', None),
        check_vma=False)
```

```python
import functools

import jax
import jax.numpy as jnp
import numpy as np
from jax import lax
from jax.experimental import pallas as pl
from jax.experimental.pallas import tpu as pltpu
from jax.sharding import PartitionSpec as P

ROPE_THETA = 500000.0
MESH = pl.DeviceIdType.MESH
F32 = jnp.float32
BF16 = jnp.bfloat16

ROWS = 32
DIM = 12288
HEADS = 6
HD = 128
SEQ = 4
KVH = 4
T_DEV = 512
TN = 2 * T_DEV
KC = 4
KD = DIM // KC
AHEAD = 7
VMEM_LIMIT = 60 * 2 ** 20
SLOTS = 8
BC = 8
NB = ROWS // BC
HALF = ROWS // 2
PITCH = 40
GROUP = 2
BLK = DIM // 8


def kernel(x_h, len_h, freq_h, k_h, v_h, wq_h, wo_h, out_ref,
           x_s, len_s, freq_s, wq_s, k_s, v_s, wo_s,
           posq, qg, q_t, ob, mlb, rb, attn_s, ypart, yrecv, yrecv2, zrecv,
           in_sem, wq_sem, k_sem, v_sem, wo_sem,
           qs_sem, qr_sem, cs_sem, cr_sem,
           ds_sem, dr_sem, ys_sem, yr_sem, zs_sem, zr_sem,
           azs_sem, azr_sem, ays_sem, ayr_sem, ads_sem, adr_sem, turn_sem):
    d = lax.axis_index('dp')
    z = lax.axis_index('kvh')
    me = lax.axis_index('seq')
    core = lax.rem(me, 2)
    y = lax.div(me, 2)

    def seq_peer(i):
        c = 1 - core if i & 1 else core
        yy = 1 - y if i & 2 else y
        return yy * 2 + c

    far = 1 - lax.div(z, 2)
    zs = [3 * far, 1 + far, z + 1 - 2 * lax.rem(z, 2), z]
    blocks = [zz * 2 + (1 - y) for zz in zs] + [zz * 2 + y for zz in zs]

    x_cp = pltpu.make_async_copy(x_h, x_s, in_sem.at[0])
    len_cp = pltpu.make_async_copy(len_h, len_s, in_sem.at[1])
    freq_cp = pltpu.make_async_copy(freq_h, freq_s, in_sem.at[2])
    len_cp.start()
    freq_cp.start()
    x_cp.start()

    def wq_cp(p, c):
        n = p * KC + c
        src = wq_h.at[pl.ds(2 * p, 2), pl.ds(c * KD, KD)]
        return pltpu.make_async_copy(src, wq_s.at[n % SLOTS], wq_sem.at[n])

    def k_cp(j):
        at = pl.ds(j * BC, BC)
        return pltpu.make_async_copy(k_h.at[at], k_s.at[at], k_sem.at[j])

    def v_cp(j):
        at = pl.ds(j * BC, BC)
        return pltpu.make_async_copy(v_h.at[at], v_s.at[at], v_sem.at[j])

    def wo_cp(i):
        src = wo_h.at[:, pl.ds(pl.multiple_of(blocks[i] * BLK, BLK), BLK)]
        return pltpu.make_async_copy(src, wo_s.at[i], wo_sem.at[i])

    fetches = [wq_cp(p, c) for p in range(3) for c in range(KC)]
    for j in range(NB):
        fetches += [k_cp(j), v_cp(j)]
    for cp in fetches[:AHEAD]:
        cp.start(priority=1)

    barrier = pltpu.get_barrier_semaphore()
    for i in range(1, SEQ):
        pl.semaphore_signal(barrier, inc=1, device_id=(d, z, seq_peer(i)), device_id_type=MESH)
    for i in range(1, KVH):
        pl.semaphore_signal(barrier, inc=1, device_id=(d, lax.rem(z + i, KVH), me), device_id_type=MESH)

    q_t[...] = jnp.zeros_like(q_t)
    lane = lax.broadcasted_iota(jnp.int32, (ROWS, TN), 1)
    row = lax.broadcasted_iota(jnp.int32, (ROWS, TN), 0)
    mine = (lane & 1) == (row >> 4)
    posq[...] = jnp.where(mine, me * T_DEV + (lane >> 1), 1 << 30)
    len_cp.wait()
    freq_cp.wait()
    rows128 = lax.broadcasted_iota(jnp.int32, (ROWS, HD), 0)
    lane128 = lax.broadcasted_iota(jnp.int32, (ROWS, HD), 1)
    pos = jnp.zeros((ROWS, HD), jnp.int32)
    for b in range(ROWS):
        pos = jnp.where(rows128 == b, len_s[b] - 1, pos)
    angle = pos.astype(F32) * freq_s[0:1, :]
    cosine = jnp.cos(angle)
    sine = jnp.sin(angle)
    sine = jnp.where(lane128 < HD // 2, -sine, sine)

    def q_copy(p, i, slot):
        at = (slot, pl.ds(2 * p, 2))
        return pltpu.make_async_remote_copy(
            src_ref=qg.at[at], dst_ref=qg.at[at],
            send_sem=qs_sem.at[p, i - 1], recv_sem=qr_sem.at[p, i - 1],
            device_id=(d, z, seq_peer(i)), device_id_type=MESH)

    x_cp.wait()
    for p in range(3):
        acc = [jnp.zeros((ROWS, HD), F32)] * 2
        for c in range(KC):
            n = p * KC + c
            wq_cp(p, c).wait()
            fetches[n + AHEAD].start(priority=1)
            at = slice(c * KD, (c + 1) * KD)
            for u in range(2):
                acc[u] = acc[u] + jnp.dot(x_s[:, at], wq_s[n % SLOTS, u], preferred_element_type=F32)
        for u in range(2):
            q = acc[u]
            q = q * cosine + pltpu.roll(q, HD // 2, axis=1) * sine
            qg[me, 2 * p + u] = q.astype(BF16)
        if p == 0:
            pl.semaphore_wait(barrier, SEQ - 1 + KVH - 1)
        for i in range(1, SEQ):
            q_copy(p, i, me).start()
    for cp in fetches[3 * KC + AHEAD:] + [wo_cp(0)]:
        cp.start(priority=1)
    for p in range(3):
        for i in range(1, SEQ):
            q_copy(p, i, seq_peer(i)).wait_recv()
    for i in range(1, 8):
        wo_cp(i).start(priority=1)
    q_rows = q_t.reshape(ROWS * PITCH, HD)
    for s in range(SEQ):
        for h in range(HEADS):
            q_rows[pl.ds(s * 8 + h, ROWS, stride=PITCH), :] = qg[s, h].astype(F32)

    ob_rows = ob.reshape(32 * ROWS, HD)
    ml_rows = mlb.reshape(ROWS * PITCH, HD)
    scale = HD ** -0.5

    def c_copy(j, i, dst, slot):
        at = pl.ds(j * BC, BC)
        return pltpu.make_async_remote_copy(
            src_ref=ob.at[at, dst], dst_ref=rb.at[slot, at],
            send_sem=cs_sem.at[j, i - 1], recv_sem=cr_sem.at[j, i - 1],
            device_id=(d, z, seq_peer(i)), device_id_type=MESH)

    lane8 = lax.broadcasted_iota(jnp.int32, (BC, HD), 1)
    lane32 = lax.broadcasted_iota(jnp.int32, (32, HD), 1)

    def piece(j, carry):
        k_cp(j).wait()
        v_cp(j).wait()
        for g in range(BC // 4):
            ws = []
            for h in range(2):
                b = j * BC + g * 4 + 2 * h
                qa, qb = q_t[b, :32].astype(BF16), q_t[b + 1, :32].astype(BF16)
                for u in range(2):
                    s = lax.dot_general(qa if u == 0 else qb, k_s[b + u], (((1,), (1,)), ((), ())), preferred_element_type=F32)
                    s = jnp.where(posq[...] < len_s[b + u], s * scale, -jnp.inf)
                    m = jnp.max(s, axis=1, keepdims=True)
                    w = jnp.exp(s - jnp.where(m == -jnp.inf, 0.0, m))
                    l = jnp.sum(w, axis=1, keepdims=True)
                    mlb[b + u, :32] = jnp.where(lane32 < 64, m, l)
                    ws.append(w.astype(BF16))
            for u in range(4):
                b = j * BC + g * 4 + u
                out = jnp.dot(ws[u], v_s[b], preferred_element_type=F32)
                for v in range(SEQ):
                    ob[b, v] = out[v * 8:(v + 1) * 8]
        for v in range(SEQ):
            stat = jnp.zeros((BC, HD), F32)
            for h in range(HEADS):
                of_head = ml_rows[pl.ds(j * BC * PITCH + v * 8 + h, BC, stride=PITCH), :]
                stat = jnp.where((lane8 & 63) == h, of_head, stat)
            ob_rows[pl.ds(j * BC * 32 + v * 8 + HEADS, BC, stride=32), :] = stat
        for i in range(1, SEQ):
            c_copy(j, i, seq_peer(i), me).start()
        return carry

    lax.fori_loop(0, NB, piece, 0)
    for p in range(3):
        for i in range(1, SEQ):
            q_copy(p, i, me).wait_send()
    def combine(half):
        for j in range(half * NB // 2, (half + 1) * NB // 2):
            for i in range(1, SEQ):
                c_copy(j, i, seq_peer(i), seq_peer(i)).wait_recv()
        at = pl.ds(half * HALF, HALF)
        rb_rows = rb.reshape(SEQ * ROWS * 8, HD)

        def part(i, h):
            if i == 0:
                return ob_rows[pl.ds(half * HALF * 32 + me * 8 + h, HALF, stride=32), :]
            return rb_rows[pl.ds((seq_peer(i) * ROWS + half * HALF) * 8 + h, HALF, stride=8), :]

        stats = [part(i, HEADS) for i in range(SEQ)]
        top = functools.reduce(jnp.maximum, stats)
        fac = [jnp.exp(st - top) for st in stats]
        total = functools.reduce(jnp.add, [f * pltpu.roll(st, 64, axis=1) for f, st in zip(fac, stats)])
        for h in range(HEADS):
            o = functools.reduce(jnp.add, [part(i, h) * f[:, h:h + 1] for i, f in enumerate(fac)])
            attn_s[at, h * HD:(h + 1) * HD] = (o / total[:, h:h + 1]).astype(BF16)

    def d_copy(half, n):
        return pltpu.make_async_remote_copy(
            src_ref=ypart.at[half, n], dst_ref=yrecv.at[n], send_sem=ds_sem.at[n], recv_sem=dr_sem.at[n],
            device_id=(d, z, seq_peer(1)), device_id_type=MESH)

    def y_copy(n):
        return pltpu.make_async_remote_copy(
            src_ref=ypart.at[core, n], dst_ref=yrecv2.at[n], send_sem=ys_sem.at[n], recv_sem=yr_sem.at[n],
            device_id=(d, z, seq_peer(2)), device_id_type=MESH)

    def z_copy(n, to, slot):
        return pltpu.make_async_remote_copy(
            src_ref=ypart.at[core, 4 + n], dst_ref=zrecv.at[slot], send_sem=zs_sem.at[n], recv_sem=zr_sem.at[slot],
            device_id=(d, to, me), device_id_type=MESH)

    def y_step(n):
        y_copy(n).wait_recv()
        ypart[core, 4 + n] = ypart[core, 4 + n] + yrecv2[n]
        if n < 3:
            z_copy(n, zs[n], z).start()

    def d_step(half, n):
        for u in range(n, n + GROUP):
            d_copy(half, u).wait_recv()
            ypart[half, u] = ypart[half, u] + yrecv[u]
            if u < 4:
                y_copy(u).start()

    for half in range(2):
        combine(half)
        for n in range(0, 8 + GROUP, GROUP):
            if n < 8:
                if half == 0:
                    for u in range(n, n + GROUP):
                        wo_cp(u).wait()
                for u in range(n, n + GROUP):
                    ypart[half, u] = jnp.dot(attn_s[half * HALF:(half + 1) * HALF, :], wo_s[u],
                                             preferred_element_type=F32)

                @pl.when(core != half)
                def _():
                    for u in range(n, n + GROUP):
                        d_copy(half, u).start()
            if 0 < n <= 4 or (n > 4 and half == 1):
                @pl.when(core == half)
                def _():
                    d_step(half, n - GROUP)
            if half == 1 and n in (2, 4):
                @pl.when(core == 0)
                def _():
                    d_step(0, n + 2)
            if half == 1 and n >= 4:
                @pl.when(core == 0)
                def _():
                    y_step((n - 4) // 2)

    @pl.when(core == 0)
    def _():
        y_step(3)

    @pl.when(core == 1)
    def _():
        for n in range(4):
            y_step(n)
        pl.semaphore_signal(turn_sem, inc=1, device_id=(d, z, seq_peer(1)), device_id_type=MESH)

    def block_at(half, block):
        return (pl.ds(pl.multiple_of(half * HALF, HALF), HALF), pl.ds(pl.multiple_of(block * BLK, BLK), BLK))

    def ag_z(i, block, to, frm):
        at = block_at(core, block)
        return pltpu.make_async_remote_copy(
            src_ref=out_ref.at[at], dst_ref=out_ref.at[at], send_sem=azs_sem.at[i], recv_sem=azr_sem.at[frm],
            device_id=(d, to, me), device_id_type=MESH)

    def ag_y(block, zz):
        at = block_at(core, block)
        return pltpu.make_async_remote_copy(
            src_ref=out_ref.at[at], dst_ref=out_ref.at[at], send_sem=ays_sem.at[zz], recv_sem=ayr_sem.at[zz],
            device_id=(d, z, seq_peer(2)), device_id_type=MESH)

    def ag_d(half, block):
        at = block_at(half, block)
        return pltpu.make_async_remote_copy(
            src_ref=out_ref.at[at], dst_ref=out_ref.at[at], send_sem=ads_sem.at[block], recv_sem=adr_sem.at[block],
            device_id=(d, z, seq_peer(1)), device_id_type=MESH)

    for n in range(3):
        z_copy(n, zs[n], zs[n]).wait_recv()
    own = z * 2 + y
    at = block_at(core, own)
    f = ypart[core, 7] + zrecv[zs[0]] + zrecv[zs[1]] + zrecv[zs[2]]
    out_ref[at] = (x_s[at].astype(F32) + f).astype(BF16)
    ag_d(core, own).start()

    @pl.when(core == 0)
    def _():
        pl.semaphore_wait(turn_sem, 1)

    az = [lax.rem(z + i, KVH) for i in (1, 3, 2)]
    for n in range(3):
        ag_z(n, own, az[n], z).start()
    ag_y(own, z).start()
    for n in (0, 1, 2):
        b = az[n] * 2 + y
        ag_z(n, b, az[n], az[n]).wait_recv()
        ag_y(b, az[n]).start()
        ag_d(core, b).start()
    for zz in (z, az[0], az[1], az[2]):
        b = zz * 2 + (1 - y)
        ag_y(b, zz).wait_recv()
        ag_d(core, b).start()
    for n in range(8):
        ag_d(1 - core, n).wait_recv()

    for j in range(NB):
        for i in range(1, SEQ):
            c_copy(j, i, seq_peer(i), me).wait_send()
    for n in range(8):
        d_copy(0, n).wait_send()
        ag_d(core, n).wait_send()
    for n in range(4):
        y_copy(n).wait_send()
        ag_y(n * 2 + y, n).wait_send()
    for n in range(3):
        z_copy(n, zs[n], z).wait_send()

    for n in range(3):
        ag_z(n, own, az[n], z).wait_send()


def solution(mesh):
    half = HD // 2
    freq = ROPE_THETA ** (-np.arange(half, dtype=np.float64) * (2.0 / HD))
    freq = np.tile(np.concatenate([freq, freq]).astype(np.float32), (8, 1))
    dma = pltpu.SemaphoreType.DMA

    def local_step(x_hidden, seq_lens, k_loc, v_loc, wq_loc, wo_loc):
        any_spec = pl.BlockSpec(memory_space=pl.ANY)
        return pl.pallas_call(
            kernel,
            out_shape=pltpu.VMEM((ROWS, DIM), BF16),
            in_specs=[any_spec] * 7,
            out_specs=pl.BlockSpec(memory_space=pltpu.VMEM),
            scratch_shapes=[
                pltpu.VMEM((ROWS, DIM), BF16),
                pltpu.SMEM((ROWS,), jnp.int32),
                pltpu.VMEM((8, HD), F32),
                pltpu.VMEM((SLOTS, 2, KD, HD), BF16),
                pltpu.VMEM((ROWS, TN, HD), BF16),
                pltpu.VMEM((ROWS, TN, HD), BF16),
                pltpu.VMEM((8, HEADS * HD, BLK), BF16),
                pltpu.VMEM((ROWS, TN), jnp.int32),
                pltpu.VMEM((SEQ, HEADS, ROWS, HD), BF16),
                pltpu.VMEM((ROWS, PITCH, HD), F32),
                pltpu.VMEM((ROWS, SEQ, 8, HD), F32),
                pltpu.VMEM((ROWS, PITCH, HD), F32),
                pltpu.VMEM((SEQ, ROWS, 8, HD), F32),
                pltpu.VMEM((ROWS, HEADS * HD), BF16),
                pltpu.VMEM((2, 8, HALF, BLK), F32),
                pltpu.VMEM((8, HALF, BLK), F32),
                pltpu.VMEM((4, HALF, BLK), F32),
                pltpu.VMEM((4, HALF, BLK), F32),
                dma((3,)), dma((3 * KC,)), dma((NB,)), dma((NB,)), dma((8,)),
                dma((3, 3)), dma((3, 3)), dma((NB, 3)), dma((NB, 3)),
                dma((8,)), dma((8,)), dma((4,)), dma((4,)), dma((3,)), dma((4,)),
                dma((3,)), dma((4,)), dma((4,)), dma((4,)), dma((8,)), dma((8,)),
                pltpu.SemaphoreType.REGULAR,
            ],
            compiler_params=pltpu.CompilerParams(
                collective_id=0, has_side_effects=True, vmem_limit_bytes=VMEM_LIMIT),
            name='decode_step',
        )(x_hidden, seq_lens, jnp.asarray(freq),
          k_loc.reshape(ROWS, TN, HD), v_loc.reshape(ROWS, TN, HD),
          wq_loc.transpose(1, 0, 2), wo_loc.reshape(HEADS * HD, DIM))

    return jax.shard_map(
        local_step,
        mesh=mesh,
        in_specs=(P('dp', None), P('dp'), P('dp', 'seq', 'kvh', None), P('dp', 'seq', 'kvh', None),
                  P(None, ('kvh', 'seq'), None), P(('kvh', 'seq'), None, None)),
        out_specs=P('dp', None),
        check_vma=False)
```

```python
import functools

import jax
import jax.numpy as jnp
import numpy as np
from jax import lax
from jax.experimental import pallas as pl
from jax.experimental.pallas import tpu as pltpu
from jax.sharding import PartitionSpec as P

ROPE_THETA = 500000.0
MESH = pl.DeviceIdType.MESH
F32 = jnp.float32
BF16 = jnp.bfloat16

ROWS = 32
DIM = 12288
HEADS = 6
HD = 128
SEQ = 4
KVH = 4
T_DEV = 512
TN = 2 * T_DEV
KC = 6
KD = DIM // KC
AHEAD = 10
VMEM_LIMIT = 60 * 2 ** 20
SLOTS = 12
BC = 8
NB = ROWS // BC
HALF = ROWS // 2
PITCH = 40
GROUP = 2
BLK = DIM // 8


def kernel(x_h, len_h, freq_h, k_h, v_h, wq_h, wo_h, out_ref,
           x_s, len_s, freq_s, wq_s, k_s, v_s, wo_s,
           posq, qg, q_t, ob, mlb, rb, attn_s, ypart, yrecv, yrecv2, zrecv,
           in_sem, wq_sem, k_sem, v_sem, wo_sem,
           qs_sem, qr_sem, cs_sem, cr_sem,
           ds_sem, dr_sem, ys_sem, yr_sem, zs_sem, zr_sem,
           azs_sem, azr_sem, ays_sem, ayr_sem, ads_sem, adr_sem, turn_sem):
    d = lax.axis_index('dp')
    z = lax.axis_index('kvh')
    me = lax.axis_index('seq')
    core = lax.rem(me, 2)
    y = lax.div(me, 2)

    def seq_peer(i):
        c = 1 - core if i & 1 else core
        yy = 1 - y if i & 2 else y
        return yy * 2 + c

    far = 1 - lax.div(z, 2)
    zs = [3 * far, 1 + far, z + 1 - 2 * lax.rem(z, 2), z]
    blocks = [zz * 2 + (1 - y) for zz in zs] + [zz * 2 + y for zz in zs]

    x_cp = pltpu.make_async_copy(x_h, x_s, in_sem.at[0])
    len_cp = pltpu.make_async_copy(len_h, len_s, in_sem.at[1])
    freq_cp = pltpu.make_async_copy(freq_h, freq_s, in_sem.at[2])
    len_cp.start()
    freq_cp.start()
    x_cp.start()

    def wq_cp(p, c):
        n = p * KC + c
        src = wq_h.at[pl.ds(2 * p, 2), pl.ds(c * KD, KD)]
        return pltpu.make_async_copy(src, wq_s.at[n % SLOTS], wq_sem.at[n])

    def k_cp(j):
        at = pl.ds(j * BC, BC)
        return pltpu.make_async_copy(k_h.at[at], k_s.at[at], k_sem.at[j])

    def v_cp(j):
        at = pl.ds(j * BC, BC)
        return pltpu.make_async_copy(v_h.at[at], v_s.at[at], v_sem.at[j])

    def wo_cp(i):
        src = wo_h.at[:, pl.ds(pl.multiple_of(blocks[i] * BLK, BLK), BLK)]
        return pltpu.make_async_copy(src, wo_s.at[i], wo_sem.at[i])

    fetches = [wq_cp(p, c) for p in range(3) for c in range(KC)]
    for j in range(NB):
        fetches += [k_cp(j), v_cp(j)]
    for cp in fetches[:AHEAD]:
        cp.start(priority=1)

    barrier = pltpu.get_barrier_semaphore()
    for i in range(1, SEQ):
        pl.semaphore_signal(barrier, inc=1, device_id=(d, z, seq_peer(i)), device_id_type=MESH)
    for i in range(1, KVH):
        pl.semaphore_signal(barrier, inc=1, device_id=(d, lax.rem(z + i, KVH), me), device_id_type=MESH)

    q_t[...] = jnp.zeros_like(q_t)
    lane = lax.broadcasted_iota(jnp.int32, (ROWS, TN), 1)
    row = lax.broadcasted_iota(jnp.int32, (ROWS, TN), 0)
    mine = (lane & 1) == (row >> 4)
    posq[...] = jnp.where(mine, me * T_DEV + (lane >> 1), 1 << 30)
    len_cp.wait()
    freq_cp.wait()
    rows128 = lax.broadcasted_iota(jnp.int32, (ROWS, HD), 0)
    lane128 = lax.broadcasted_iota(jnp.int32, (ROWS, HD), 1)
    pos = jnp.zeros((ROWS, HD), jnp.int32)
    for b in range(ROWS):
        pos = jnp.where(rows128 == b, len_s[b] - 1, pos)
    angle = pos.astype(F32) * freq_s[0:1, :]
    cosine = jnp.cos(angle)
    sine = jnp.sin(angle)
    sine = jnp.where(lane128 < HD // 2, -sine, sine)

    def q_copy(p, i, slot):
        at = (slot, pl.ds(2 * p, 2))
        return pltpu.make_async_remote_copy(
            src_ref=qg.at[at], dst_ref=qg.at[at],
            send_sem=qs_sem.at[p, i - 1], recv_sem=qr_sem.at[p, i - 1],
            device_id=(d, z, seq_peer(i)), device_id_type=MESH)

    x_cp.wait()
    for p in range(3):
        acc = [jnp.zeros((ROWS, HD), F32)] * 2
        for c in range(KC):
            n = p * KC + c
            wq_cp(p, c).wait()
            if n + AHEAD < len(fetches):
                fetches[n + AHEAD].start(priority=1)
            at = slice(c * KD, (c + 1) * KD)
            for u in range(2):
                acc[u] = acc[u] + jnp.dot(x_s[:, at], wq_s[n % SLOTS, u], preferred_element_type=F32)
        for u in range(2):
            q = acc[u]
            q = q * cosine + pltpu.roll(q, HD // 2, axis=1) * sine
            qg[me, 2 * p + u] = q.astype(BF16)
        if p == 0:
            pl.semaphore_wait(barrier, SEQ - 1 + KVH - 1)
        for i in range(1, SEQ):
            q_copy(p, i, me).start()
    for cp in fetches[3 * KC + AHEAD:] + [wo_cp(0)]:
        cp.start(priority=1)
    for p in range(3):
        for i in range(1, SEQ):
            q_copy(p, i, seq_peer(i)).wait_recv()
    for i in range(1, 8):
        wo_cp(i).start(priority=1)
    q_rows = q_t.reshape(ROWS * PITCH, HD)
    for s in range(SEQ):
        for h in range(HEADS):
            q_rows[pl.ds(s * 8 + h, ROWS, stride=PITCH), :] = qg[s, h].astype(F32)

    ob_rows = ob.reshape(32 * ROWS, HD)
    ml_rows = mlb.reshape(ROWS * PITCH, HD)
    scale = HD ** -0.5

    def c_copy(j, i, dst, slot):
        at = pl.ds(j * BC, BC)
        return pltpu.make_async_remote_copy(
            src_ref=ob.at[at, dst], dst_ref=rb.at[slot, at],
            send_sem=cs_sem.at[j, i - 1], recv_sem=cr_sem.at[j, i - 1],
            device_id=(d, z, seq_peer(i)), device_id_type=MESH)

    lane8 = lax.broadcasted_iota(jnp.int32, (BC, HD), 1)
    lane32 = lax.broadcasted_iota(jnp.int32, (32, HD), 1)

    def piece(j, carry):
        k_cp(j).wait()
        v_cp(j).wait()
        for g in range(BC // 4):
            ws = []
            for h in range(2):
                b = j * BC + g * 4 + 2 * h
                qa, qb = q_t[b, :32].astype(BF16), q_t[b + 1, :32].astype(BF16)
                for u in range(2):
                    s = lax.dot_general(qa if u == 0 else qb, k_s[b + u], (((1,), (1,)), ((), ())), preferred_element_type=F32)
                    s = jnp.where(posq[...] < len_s[b + u], s * scale, -jnp.inf)
                    m = jnp.max(s, axis=1, keepdims=True)
                    w = jnp.exp(s - jnp.where(m == -jnp.inf, 0.0, m))
                    l = jnp.sum(w, axis=1, keepdims=True)
                    mlb[b + u, :32] = jnp.where(lane32 < 64, m, l)
                    ws.append(w.astype(BF16))
            for u in range(4):
                b = j * BC + g * 4 + u
                out = jnp.dot(ws[u], v_s[b], preferred_element_type=F32)
                for v in range(SEQ):
                    ob[b, v] = out[v * 8:(v + 1) * 8]
        for v in range(SEQ):
            stat = jnp.zeros((BC, HD), F32)
            for h in range(HEADS):
                of_head = ml_rows[pl.ds(j * BC * PITCH + v * 8 + h, BC, stride=PITCH), :]
                stat = jnp.where((lane8 & 63) == h, of_head, stat)
            ob_rows[pl.ds(j * BC * 32 + v * 8 + HEADS, BC, stride=32), :] = stat
        for i in range(1, SEQ):
            c_copy(j, i, seq_peer(i), me).start()
        return carry

    lax.fori_loop(0, NB, piece, 0)
    for p in range(3):
        for i in range(1, SEQ):
            q_copy(p, i, me).wait_send()
    def combine(half):
        for j in range(half * NB // 2, (half + 1) * NB // 2):
            for i in range(1, SEQ):
                c_copy(j, i, seq_peer(i), seq_peer(i)).wait_recv()
        at = pl.ds(half * HALF, HALF)
        rb_rows = rb.reshape(SEQ * ROWS * 8, HD)

        def part(i, h):
            if i == 0:
                return ob_rows[pl.ds(half * HALF * 32 + me * 8 + h, HALF, stride=32), :]
            return rb_rows[pl.ds((seq_peer(i) * ROWS + half * HALF) * 8 + h, HALF, stride=8), :]

        stats = [part(i, HEADS) for i in range(SEQ)]
        top = functools.reduce(jnp.maximum, stats)
        fac = [jnp.exp(st - top) for st in stats]
        total = functools.reduce(jnp.add, [f * pltpu.roll(st, 64, axis=1) for f, st in zip(fac, stats)])
        for h in range(HEADS):
            o = functools.reduce(jnp.add, [part(i, h) * f[:, h:h + 1] for i, f in enumerate(fac)])
            attn_s[at, h * HD:(h + 1) * HD] = (o / total[:, h:h + 1]).astype(BF16)

    def d_copy(half, n):
        return pltpu.make_async_remote_copy(
            src_ref=ypart.at[half, n], dst_ref=yrecv.at[n], send_sem=ds_sem.at[n], recv_sem=dr_sem.at[n],
            device_id=(d, z, seq_peer(1)), device_id_type=MESH)

    def y_copy(n):
        return pltpu.make_async_remote_copy(
            src_ref=ypart.at[core, n], dst_ref=yrecv2.at[n], send_sem=ys_sem.at[n], recv_sem=yr_sem.at[n],
            device_id=(d, z, seq_peer(2)), device_id_type=MESH)

    def z_copy(n, to, slot):
        return pltpu.make_async_remote_copy(
            src_ref=ypart.at[core, 4 + n], dst_ref=zrecv.at[slot], send_sem=zs_sem.at[n], recv_sem=zr_sem.at[slot],
            device_id=(d, to, me), device_id_type=MESH)

    def y_step(n):
        y_copy(n).wait_recv()
        ypart[core, 4 + n] = ypart[core, 4 + n] + yrecv2[n]
        if n < 3:
            z_copy(n, zs[n], z).start()

    def d_step(half, n):
        for u in range(n, n + GROUP):
            d_copy(half, u).wait_recv()
            ypart[half, u] = ypart[half, u] + yrecv[u]
            if u < 4:
                y_copy(u).start()

    for half in range(2):
        combine(half)
        for n in range(0, 8 + GROUP, GROUP):
            if n < 8:
                if half == 0:
                    for u in range(n, n + GROUP):
                        wo_cp(u).wait()
                for u in range(n, n + GROUP):
                    ypart[half, u] = jnp.dot(attn_s[half * HALF:(half + 1) * HALF, :], wo_s[u],
                                             preferred_element_type=F32)

                @pl.when(core != half)
                def _():
                    for u in range(n, n + GROUP):
                        d_copy(half, u).start()
            if 0 < n <= 4 or (n > 4 and half == 1):
                @pl.when(core == half)
                def _():
                    d_step(half, n - GROUP)
            if half == 1 and n in (2, 4):
                @pl.when(core == 0)
                def _():
                    d_step(0, n + 2)
            if half == 1 and n >= 4:
                @pl.when(core == 0)
                def _():
                    y_step((n - 4) // 2)

    @pl.when(core == 0)
    def _():
        y_step(3)

    @pl.when(core == 1)
    def _():
        for n in range(4):
            y_step(n)
        pl.semaphore_signal(turn_sem, inc=1, device_id=(d, z, seq_peer(1)), device_id_type=MESH)

    def block_at(half, block):
        return (pl.ds(pl.multiple_of(half * HALF, HALF), HALF), pl.ds(pl.multiple_of(block * BLK, BLK), BLK))

    def ag_z(i, block, to, frm):
        at = block_at(core, block)
        return pltpu.make_async_remote_copy(
            src_ref=out_ref.at[at], dst_ref=out_ref.at[at], send_sem=azs_sem.at[i], recv_sem=azr_sem.at[frm],
            device_id=(d, to, me), device_id_type=MESH)

    def ag_y(block, zz):
        at = block_at(core, block)
        return pltpu.make_async_remote_copy(
            src_ref=out_ref.at[at], dst_ref=out_ref.at[at], send_sem=ays_sem.at[zz], recv_sem=ayr_sem.at[zz],
            device_id=(d, z, seq_peer(2)), device_id_type=MESH)

    def ag_d(half, block):
        at = block_at(half, block)
        return pltpu.make_async_remote_copy(
            src_ref=out_ref.at[at], dst_ref=out_ref.at[at], send_sem=ads_sem.at[block], recv_sem=adr_sem.at[block],
            device_id=(d, z, seq_peer(1)), device_id_type=MESH)

    for n in range(3):
        z_copy(n, zs[n], zs[n]).wait_recv()
    own = z * 2 + y
    at = block_at(core, own)
    f = ypart[core, 7] + zrecv[zs[0]] + zrecv[zs[1]] + zrecv[zs[2]]
    out_ref[at] = (x_s[at].astype(F32) + f).astype(BF16)
    ag_d(core, own).start()

    @pl.when(core == 0)
    def _():
        pl.semaphore_wait(turn_sem, 1)

    az = [lax.rem(z + i, KVH) for i in (1, 3, 2)]
    for n in range(3):
        ag_z(n, own, az[n], z).start()
    ag_y(own, z).start()
    for n in (0, 1, 2):
        b = az[n] * 2 + y
        ag_z(n, b, az[n], az[n]).wait_recv()
        ag_y(b, az[n]).start()
        ag_d(core, b).start()
    for zz in (z, az[0], az[1], az[2]):
        b = zz * 2 + (1 - y)
        ag_y(b, zz).wait_recv()
        ag_d(core, b).start()
    for n in range(8):
        ag_d(1 - core, n).wait_recv()

    for j in range(NB):
        for i in range(1, SEQ):
            c_copy(j, i, seq_peer(i), me).wait_send()
    for n in range(8):
        d_copy(0, n).wait_send()
        ag_d(core, n).wait_send()
    for n in range(4):
        y_copy(n).wait_send()
        ag_y(n * 2 + y, n).wait_send()
    for n in range(3):
        z_copy(n, zs[n], z).wait_send()

    for n in range(3):
        ag_z(n, own, az[n], z).wait_send()


def solution(mesh):
    half = HD // 2
    freq = ROPE_THETA ** (-np.arange(half, dtype=np.float64) * (2.0 / HD))
    freq = np.tile(np.concatenate([freq, freq]).astype(np.float32), (8, 1))
    dma = pltpu.SemaphoreType.DMA

    def local_step(x_hidden, seq_lens, k_loc, v_loc, wq_loc, wo_loc):
        any_spec = pl.BlockSpec(memory_space=pl.ANY)
        return pl.pallas_call(
            kernel,
            out_shape=pltpu.VMEM((ROWS, DIM), BF16),
            in_specs=[any_spec] * 7,
            out_specs=pl.BlockSpec(memory_space=pltpu.VMEM),
            scratch_shapes=[
                pltpu.VMEM((ROWS, DIM), BF16),
                pltpu.SMEM((ROWS,), jnp.int32),
                pltpu.VMEM((8, HD), F32),
                pltpu.VMEM((SLOTS, 2, KD, HD), BF16),
                pltpu.VMEM((ROWS, TN, HD), BF16),
                pltpu.VMEM((ROWS, TN, HD), BF16),
                pltpu.VMEM((8, HEADS * HD, BLK), BF16),
                pltpu.VMEM((ROWS, TN), jnp.int32),
                pltpu.VMEM((SEQ, HEADS, ROWS, HD), BF16),
                pltpu.VMEM((ROWS, PITCH, HD), F32),
                pltpu.VMEM((ROWS, SEQ, 8, HD), F32),
                pltpu.VMEM((ROWS, PITCH, HD), F32),
                pltpu.VMEM((SEQ, ROWS, 8, HD), F32),
                pltpu.VMEM((ROWS, HEADS * HD), BF16),
                pltpu.VMEM((2, 8, HALF, BLK), F32),
                pltpu.VMEM((8, HALF, BLK), F32),
                pltpu.VMEM((4, HALF, BLK), F32),
                pltpu.VMEM((4, HALF, BLK), F32),
                dma((3,)), dma((3 * KC,)), dma((NB,)), dma((NB,)), dma((8,)),
                dma((3, 3)), dma((3, 3)), dma((NB, 3)), dma((NB, 3)),
                dma((8,)), dma((8,)), dma((4,)), dma((4,)), dma((3,)), dma((4,)),
                dma((3,)), dma((4,)), dma((4,)), dma((4,)), dma((8,)), dma((8,)),
                pltpu.SemaphoreType.REGULAR,
            ],
            compiler_params=pltpu.CompilerParams(
                collective_id=0, has_side_effects=True, vmem_limit_bytes=VMEM_LIMIT),
            name='decode_step',
        )(x_hidden, seq_lens, jnp.asarray(freq),
          k_loc.reshape(ROWS, TN, HD), v_loc.reshape(ROWS, TN, HD),
          wq_loc.transpose(1, 0, 2), wo_loc.reshape(HEADS * HD, DIM))

    return jax.shard_map(
        local_step,
        mesh=mesh,
        in_specs=(P('dp', None), P('dp'), P('dp', 'seq', 'kvh', None), P('dp', 'seq', 'kvh', None),
                  P(None, ('kvh', 'seq'), None), P(('kvh', 'seq'), None, None)),
        out_specs=P('dp', None),
        check_vma=False)
```
